32 devices in a mesh: dom: 8 (over z, y), orb: 4 (over x, core).
Axes of the slice: x: 2, y: 2, z: 4, core: 2. Of those that a mesh axis runs over, the one named last changes fastest.
Arguments:
- orbitals: bfloat16 [16, 4, 1024, 512], P('dom', None, None, 'orb'), may hold values from -6 to 6
- slot_ids: int32 [16, 4], P('dom'), may hold values from 0 to 15, as said below
- slot_count: int32 [16], P('dom'), may hold values from 1 to 4, as said below
- band_tiles: bfloat16 [16, 3, 512, 512], P(None, None, 'dom', 'orb'), may hold values from -0.15625 to 0.15625
- pattern: int32 [16, 3], replicated, may hold values 0 or 1
- occupation: float32 [16, 512], P(None, 'orb'), may hold values from 0.0005 to 0.005
Outputs:
- rotated: bfloat16 [16, 4, 1024, 512], P('dom', None, None, 'orb')
- density: float32 [16, 1024], P('dom')
The draws below stay inside these ranges and needn't reach their ends.
Inputs may be any that keep to these rules, and one draw needn't show every extreme that they name: `slot_ids`: each row names 4 consecutive orbital blocks counted modulo 16: slot l holds (s + l) mod 16, where the first block s of a grid block may be any of the 16 blocks. The slots in use on grid block g are its first slot_count[g]; some grid block uses all 4.
All inputs are finite; a program needn't handle non-finite values.
Results may differ from the reference program's by a relative error of at most 0.00094.
Values may be sent and summed in bfloat16 or wider, within the bound.
A program may use at most 128 MiB of HBM per device.

```python
import math
import jax
import jax.numpy as jnp
from jax import lax

NB = 16
OB = 512
BAND = 3
L = 4
P_SIZE = 1024
G = 16


def draw_slot_ids(key, part):
    lowest = jax.random.randint(jax.random.fold_in(key, 11), (G,), 0, NB, dtype=jnp.int32)
    return ((lowest[:, None] + jnp.arange(L, dtype=jnp.int32)[None, :]) % NB).astype(jnp.int32)


def draw_slot_count(key, part):
    first_draw = jax.random.randint(jax.random.fold_in(key, 21), (G,), 0, L, dtype=jnp.int32)
    second = jax.random.randint(jax.random.fold_in(key, 22), (G,), 0, 2, dtype=jnp.int32)
    in_use = 1 + first_draw * second
    return jnp.where(jnp.arange(G, dtype=jnp.int32) == 0, L, in_use).astype(jnp.int32)


def touch_ends(drawn, key, least, largest):
    longest = drawn.shape.index(max(drawn.shape))
    spots = []
    for shift in (0, 1):
        where = [jax.random.randint(jax.random.fold_in(key, axis), (), 0, length) for axis, length in enumerate(drawn.shape)]
        where[longest] = (where[longest] + shift) % drawn.shape[longest]
        spots.append(tuple(where))
    return drawn.at[spots[0]].set(least).at[spots[1]].set(largest)


def shard_levels(key, dims, pieces, least, top_value):
    loudness = 1.0
    for position, parts in pieces:
        draws = jax.random.uniform(jax.random.fold_in(jax.random.fold_in(key, 6), position), (parts,), jnp.float32, least / len(pieces), top_value / len(pieces))
        loudness = loudness * jnp.repeat(jnp.exp(draws), dims[position] // parts).reshape((-1,) + (1,) * (len(dims) - 1 - position))
    return loudness


def normal_values(stream_key, dims, deviation, reach, pieces=(), kind=jnp.bfloat16):
    values = deviation * jax.random.normal(stream_key, dims, jnp.float32)
    if pieces:
        values = values * shard_levels(stream_key, dims, pieces, -0.22, 0.18)
    return jnp.clip(values, -reach, reach).astype(kind)


def setup_inputs(seed: int = 0) -> dict:
    key_list = jax.random.split(jax.random.key(seed), 7)
    return {
        "orbitals": normal_values(key_list[0], (G, L, P_SIZE, OB), 1.0, 6.0, ((0, 8), (3, 4))),
        "slot_ids": draw_slot_ids(jax.random.fold_in(key_list[6], 71), 0),
        "slot_count": draw_slot_count(jax.random.fold_in(key_list[6], 71), 0),
        "band_tiles": normal_values(key_list[3], (NB, BAND, OB, OB), (OB * BAND) ** -0.5, 0.15625, ((2, 8), (3, 4))),
        "pattern": touch_ends((jax.random.randint(key_list[4], (NB, BAND), 0, 4) < 3).astype(jnp.int32), jax.random.fold_in(key_list[4], 1), 0, 1),
        "occupation": jnp.clip(jnp.exp(math.log(0.005) - 2.30258502 * jax.random.uniform(key_list[5], (NB, OB), jnp.float32) ** shard_levels(key_list[5], (NB, OB), ((1, 4),), -0.2, 0.2)), 0.0005, 0.005),
    }


def select_tiles(band_tiles, pattern, block_ids, block_count):
    slots_per = block_ids.shape[0]
    band_count = pattern.shape[1]
    half_band = (band_count - 1) // 2
    active = jnp.arange(slots_per, dtype=jnp.int32) < block_count
    source = block_ids[:, None]
    target = block_ids[None, :]
    offset = target - source + half_band
    inside = (offset >= 0) & (offset < band_count)
    column = jnp.clip(offset, 0, band_count - 1).astype(jnp.int32)
    keeping = inside & (pattern[source, column] == 1) & active[:, None] & active[None, :]
    picked = band_tiles[source, column]
    return jnp.where(keeping[:, :, None, None], picked, jnp.zeros((), picked.dtype))


def reference(orbitals, slot_ids, slot_count, band_tiles, pattern, occupation):
    def one_block(block_items):
        values, block_ids, block_count = block_items
        tile_set = select_tiles(band_tiles, pattern, block_ids, block_count)
        rotated = jnp.einsum('lpi,lmij->mpj', values.astype(jnp.float32), tile_set.astype(jnp.float32), precision=lax.Precision.HIGHEST).astype(jnp.bfloat16)
        weights = occupation[block_ids]
        square = rotated.astype(jnp.float32) * rotated.astype(jnp.float32)
        density = jnp.einsum('mpj,mj->p', square, weights, precision=lax.Precision.HIGHEST)
        return rotated, density

    rotated, density = lax.map(one_block, (orbitals, slot_ids, slot_count))
    return (rotated, density)
```

```python
import functools
import jax
import jax.numpy as jnp
from jax import lax
from jax.experimental import pallas as pl
from jax.experimental.pallas import tpu as pltpu
from jax.sharding import PartitionSpec as P

MESH = pl.DeviceIdType.MESH
CHUNKS = 4


def grid_of(mesh):
    devices = mesh.devices
    try:
        at = [tuple(d.coords) for d in devices[:, 0]]
        width = 1
        axis = [a != b for a, b in zip(at[0], at[1])].index(True)
        while width < len(at) and all(
            at[width][i] == at[0][i] + (width if i == axis else 0) for i in range(len(at[0]))
        ):
            width += 1
        first = tuple(devices[0, 0].coords)
        cores = sum(tuple(d.coords) == first for d in devices[0, :])
    except (AttributeError, IndexError, ValueError):
        width, cores = 1, 1
    if devices.shape[0] % width:
        width = 1
    if devices.shape[1] % cores:
        cores = 1
    return width, cores


def plan_chunks(total, height, width):
    first = (width - 1, (height - 1) * width)
    rest = ((width - 1) * height, height - 1)
    best = min(
        range(0, total),
        key=lambda n: max(first[i] * n + rest[i] * (total - n) for i in (0, 1)),
    ) if width > 1 else 0
    best = max(best, 1)
    chunks = [(0, best)]
    left, start = total - best, best
    for i in range(CHUNKS):
        count = left // CHUNKS + (1 if i < left % CHUNKS else 0)
        if count:
            chunks.append((start, count))
        start += count
    return chunks


def kernel(sizes, chunks, orb_hbm, tile_hbm, ids_ref, count_ref, pat_ref, occ_ref,
           out_ref, dens_ref, tiles, obuf, wcat, dbuf, acc_ref,
           own_sem, t_send, t_recv, o_send, o_recv, d_send, d_recv):
    height, width, chips, cores = sizes
    n_tile, n_dom, rows, cols = tiles.shape
    n_orb, n_blk, slots, points, _ = obuf.shape
    band = pat_ref.shape[1]
    half = (band - 1) // 2
    dom = lax.axis_index("dom")
    orb = lax.axis_index("orb")
    h, w = dom // width, dom % width
    x, core = orb // cores, orb % cores

    load_t = pltpu.make_async_copy(tile_hbm.at[pl.ds(half, n_tile)], tiles.at[:, dom], own_sem.at[0])
    load_t.start()
    load_o = pltpu.make_async_copy(orb_hbm, obuf.at[orb], own_sem.at[1])
    load_o.start()

    can = [h + 1 < height, h > 0, w + 1 < width, w > 0]
    to = [dom + width, dom - width, dom + 1, dom - 1]

    barrier = pltpu.get_barrier_semaphore()
    expect = n_orb - 1
    for d in range(4):
        @pl.when(can[d])
        def _(d=d):
            pl.semaphore_signal(barrier, inc=1, device_id={"dom": to[d]}, device_id_type=MESH)
        expect = expect + can[d].astype(jnp.int32)
    for d in range(1, n_orb):
        pl.semaphore_signal(barrier, inc=1, device_id={"orb": (orb + d) % n_orb}, device_id_type=MESH)
    pl.semaphore_wait(barrier, expect)
    load_t.wait()

    def tile_copy(c, origin, d):
        start, count = chunks[c]
        part = tiles.at[pl.ds(start, count), origin]
        return pltpu.make_async_remote_copy(
            src_ref=part, dst_ref=part, send_sem=t_send.at[d, c, origin],
            recv_sem=t_recv.at[c, origin], device_id={"dom": to[d]}, device_id_type=MESH)

    def forward(c, origin, dirs):
        for d in dirs:
            @pl.when(can[d])
            def _(d=d):
                tile_copy(c, origin, d).start()

    def settle(c, origin, dirs):
        for d in dirs:
            @pl.when(can[d])
            def _(d=d):
                tile_copy(c, origin, d).wait_send()

    def arrive(c, origin):
        tile_copy(c, origin, 0).wait_recv()

    def orb_copy(k, origin, target):
        part = obuf.at[origin, k // slots, k % slots]
        return pltpu.make_async_remote_copy(
            src_ref=part, dst_ref=part, send_sem=o_send.at[origin, target, k],
            recv_sem=o_recv.at[origin, k], device_id={"orb": target}, device_id_type=MESH)

    n_orb_chunk = n_blk * slots
    far = [((x + i) % chips) * cores + core for i in range(1, chips)]
    near = [x * cores + (core + i) % cores for i in range(1, cores)]

    n_chunk = len(chunks)
    for c in range(n_chunk):
        forward(c, dom, (2, 3, 0, 1) if c == 0 else (0, 1, 2, 3))
    load_o.wait()
    for k in range(n_orb_chunk):
        for target in far:
            orb_copy(k, orb, target).start()
    for k in range(n_orb_chunk):
        for target in near:
            orb_copy(k, orb, target).start()

    def relay_orb(k):
        for origin in far:
            orb_copy(k, origin, orb).wait_recv()
            for target in near:
                orb_copy(k, origin, target).start()

    def along_width(act_plus, act_minus):
        def step(u, carry):
            @pl.when(w - u >= 0)
            def _():
                act_plus(w - u)
            @pl.when(w + u < width)
            def _():
                act_minus(w + u)
            return carry
        lax.fori_loop(1, width, step, 0)

    def first_in(ow, d):
        arrive(0, h * width + ow)
        forward(0, h * width + ow, (d, 0, 1))

    along_width(lambda ow: first_in(ow, 2), lambda ow: first_in(ow, 3))

    n_rest = n_chunk - 1
    lag = 2

    def height_step(t, carry):
        sides = ((h - t >= 0, h - t, 0), (h + t < height, h + t, 1))
        for ok, row, d in sides:
            @pl.when(ok)
            def _(row=row, d=d):
                arrive(0, row * width + w)
                forward(0, row * width + w, (d,))
        for c in range(1, n_chunk):
            for ok, row, d in sides:
                @pl.when(ok)
                def _(row=row, d=d, c=c):
                    arrive(c, row * width + w)
                    forward(c, row * width + w, (d, 2, 3))
            k = (t - 1) * n_rest + (c - 1) - lag
            @pl.when((k >= 0) & (k < n_orb_chunk))
            def _(k=k):
                relay_orb(k)
        for ok, row, d in sides:
            def other(u, carry, row=row, d=d):
                origin = row * width + (w + u) % width
                arrive(0, origin)
                forward(0, origin, (d,))
                return carry
            @pl.when(ok)
            def _(other=other):
                lax.fori_loop(1, width, other, 0)
        return carry

    lax.fori_loop(1, height, height_step, 0)
    done = max(0, (height - 1) * n_rest - lag)
    for k in range(min(done, n_orb_chunk), n_orb_chunk):
        relay_orb(k)

    def late_row(i, carry):
        row = (h + i) % height
        for c in range(1, n_chunk):
            def late(ow, d, c=c):
                arrive(c, row * width + ow)
                forward(c, row * width + ow, (d,))
            along_width(functools.partial(late, d=2), functools.partial(late, d=3))
        return carry

    def orb_in(k, carry):
        for target in near:
            orb_copy(k, target, orb).wait_recv()
            for i in range(1, chips):
                origin = ((x + i) % chips) * cores + target % cores
                orb_copy(k, origin, orb).wait_recv()
        return carry
    lax.fori_loop(0, n_orb_chunk, orb_in, 0)
    lax.fori_loop(0, height, late_row, 0)

    zero = jnp.zeros((), jnp.bfloat16)
    for g in range(n_blk):
        ids = [ids_ref[g, m] for m in range(slots)]
        live = [count_ref[g] > m for m in range(slots)]
        for m0 in range(0, slots, 2):
            targets = [m for m in (m0, m0 + 1) if m < slots]
            sources = [l for l in range(slots) if any(abs(l - m) <= half for m in targets)]
            for si, l in enumerate(sources):
                for ti, m in enumerate(targets):
                    at = (pl.ds(si * n_dom * rows, n_dom * rows), pl.ds(ti * cols, cols))
                    if abs(l - m) > half:
                        wcat[at[0], at[1]] = jnp.zeros((n_dom * rows, cols), jnp.bfloat16)
                        continue
                    offset = ids[m] - ids[l] + half
                    column = jnp.clip(offset, 0, band - 1)
                    keep = (offset >= 0) & (offset < band) & live[l] & live[m] & (pat_ref[ids[l], column] == 1)
                    index = jnp.clip(ids[l] * band + column - half, 0, n_tile - 1)
                    picked = tiles[index].reshape(n_dom * rows, cols)
                    wcat[at[0], at[1]] = jnp.where(keep, picked, jnp.zeros_like(picked))
            depth = len(sources) * n_dom * rows
            block = min(256, points)

            def piece(i, carry, g=g, m0=m0, targets=targets, sources=sources, depth=depth):
                span = pl.ds(pl.multiple_of(i * block, block), block)
                lhs = jnp.concatenate(
                    [obuf[o, g, l, span, :] for l in sources for o in range(n_orb)], axis=1)
                both = jnp.dot(lhs, wcat[pl.ds(0, depth), :], preferred_element_type=jnp.float32)
                total = None
                for ti, m in enumerate(targets):
                    part = both[:, ti * cols:(ti + 1) * cols].astype(jnp.bfloat16)
                    out_ref[g, m, span, :] = part
                    wide = part.astype(jnp.float32)
                    term = wide * wide * occ_ref[pl.ds(ids_ref[g, m], 1), :]
                    total = term if total is None else total + term
                if m0 > 0:
                    total = total + acc_ref[span, :]
                acc_ref[span, :] = total
                return carry
            lax.fori_loop(0, points // block, piece, 0)
        ones = jnp.ones((8, cols), jnp.float32)
        line = lax.dot_general(ones, acc_ref[...], (((1,), (1,)), ((), ())),
                               precision=lax.Precision.HIGHEST, preferred_element_type=jnp.float32)
        dbuf[orb, pl.ds(g, 1), :] = line[0:1, :]

    def settle_all(origin, carry):
        row, ow = origin // width, origin % width
        for c in range(n_chunk):
            if c == 0:
                dirs = ((row <= h, 0), (row >= h, 1), ((row == h) & (ow <= w), 2), ((row == h) & (ow >= w), 3))
            else:
                dirs = (((ow == w) & (row <= h), 0), ((ow == w) & (row >= h), 1), (ow <= w, 2), (ow >= w, 3))
            for sent, d in dirs:
                @pl.when(sent & can[d])
                def _(c=c, d=d):
                    tile_copy(c, origin, d).wait_send()
        return carry
    lax.fori_loop(0, n_dom, settle_all, 0)

    def settle_orb(k, carry):
        for target in far + near:
            orb_copy(k, orb, target).wait_send()
        for origin in far:
            for target in near:
                orb_copy(k, origin, target).wait_send()
        return carry
    lax.fori_loop(0, n_orb_chunk, settle_orb, 0)

    def dens_copy(origin, target):
        return pltpu.make_async_remote_copy(
            src_ref=dbuf.at[origin], dst_ref=dbuf.at[origin], send_sem=d_send.at[target],
            recv_sem=d_recv.at[origin], device_id={"orb": target}, device_id_type=MESH)
    for i in range(1, n_orb):
        dens_copy(orb, (orb + i) % n_orb).start()
    for i in range(1, n_orb):
        dens_copy((orb + i) % n_orb, orb).wait_recv()
    total = dbuf[0]
    for o in range(1, n_orb):
        total = total + dbuf[o]
    dens_ref[...] = total
    for i in range(1, n_orb):
        dens_copy(orb, (orb + i) % n_orb).wait_send()


def solution(mesh):
    n_dom, n_orb = mesh.shape["dom"], mesh.shape["orb"]
    width, cores = grid_of(mesh)
    height, chips = n_dom // width, n_orb // cores

    def local(orbitals, slot_ids, slot_count, band_tiles, pattern, occupation):
        n_blk, slots, points, cols = orbitals.shape
        blocks, band, rows, _ = band_tiles.shape
        half = (band - 1) // 2
        n_tile = blocks * band - 2 * half
        chunks = plan_chunks(n_tile, height, width)
        n_k = n_blk * slots
        depth = min(slots, 2 * half + 2) * n_dom * rows
        dma = pltpu.SemaphoreType.DMA
        vmem = pl.BlockSpec(memory_space=pltpu.VMEM)
        smem = pl.BlockSpec(memory_space=pltpu.SMEM)
        hbm = pl.BlockSpec(memory_space=pltpu.HBM)
        return pl.pallas_call(
            functools.partial(kernel, (height, width, chips, cores), chunks),
            out_shape=(
                jax.ShapeDtypeStruct(orbitals.shape, jnp.bfloat16),
                jax.ShapeDtypeStruct((n_blk, points), jnp.float32),
            ),
            in_specs=[hbm, hbm, smem, smem, smem, vmem],
            out_specs=(vmem, vmem),
            scratch_shapes=[
                pltpu.VMEM((n_tile, n_dom, rows, cols), jnp.bfloat16),
                pltpu.VMEM((n_orb, n_blk, slots, points, cols), jnp.bfloat16),
                pltpu.VMEM((depth, 2 * cols), jnp.bfloat16),
                pltpu.VMEM((n_orb, n_blk, points), jnp.float32),
                pltpu.VMEM((points, cols), jnp.float32),
                dma((2,)),
                dma((4, len(chunks), n_dom)),
                dma((len(chunks), n_dom)),
                dma((n_orb, n_orb, n_k)),
                dma((n_orb, n_k)),
                dma((n_orb,)),
                dma((n_orb,)),
            ],
            compiler_params=pltpu.CompilerParams(
                collective_id=0, has_side_effects=True, vmem_limit_bytes=48 * 1024 * 1024),
        )(orbitals, band_tiles.reshape(blocks * band, rows, cols), slot_ids, slot_count, pattern, occupation)

    placed = (
        P("dom", None, None, "orb"),
        P("dom", None),
        P("dom"),
        P(None, None, "dom", "orb"),
        P(),
        P(None, "orb"),
    )
    return jax.shard_map(
        local,
        mesh=mesh,
        in_specs=placed,
        out_specs=(P("dom", None, None, "orb"), P("dom", None)),
        check_vma=False,
    )
```

```python
import functools
import jax
import jax.numpy as jnp
from jax import lax
from jax.experimental import pallas as pl
from jax.experimental.pallas import tpu as pltpu
from jax.sharding import PartitionSpec as P

MESH = pl.DeviceIdType.MESH
CHUNKS = 4


def grid_of(mesh):
    devices = mesh.devices
    try:
        at = [tuple(d.coords) for d in devices[:, 0]]
        width = 1
        axis = [a != b for a, b in zip(at[0], at[1])].index(True)
        while width < len(at) and all(
            at[width][i] == at[0][i] + (width if i == axis else 0) for i in range(len(at[0]))
        ):
            width += 1
        first = tuple(devices[0, 0].coords)
        cores = sum(tuple(d.coords) == first for d in devices[0, :])
    except (AttributeError, IndexError, ValueError):
        width, cores = 1, 1
    if devices.shape[0] % width:
        width = 1
    if devices.shape[1] % cores:
        cores = 1
    return width, cores


def plan_chunks(total, height, width):
    first = (width - 1, (height - 1) * width)
    rest = ((width - 1) * height, height - 1)
    best = min(
        range(0, total),
        key=lambda n: max(first[i] * n + rest[i] * (total - n) for i in (0, 1)),
    ) if width > 1 else 0
    best = max(best, 1)
    chunks = [(0, best)]
    left, start = total - best, best
    for i in range(CHUNKS):
        count = left // CHUNKS + (1 if i < left % CHUNKS else 0)
        if count:
            chunks.append((start, count))
        start += count
    return chunks


def kernel(sizes, chunks, orb_hbm, tile_hbm, ids_ref, count_ref, pat_ref, occ_ref,
           out_ref, dens_ref, tiles, obuf, wcat, dbuf, acc_ref,
           own_sem, t_send, t_recv, o_send, o_recv, d_send, d_recv):
    height, width, chips, cores = sizes
    n_dom, n_tile, rows, cols = tiles.shape
    n_orb, n_blk, slots, points, _ = obuf.shape
    band = pat_ref.shape[0]
    half = (band - 1) // 2
    dom = lax.axis_index("dom")
    orb = lax.axis_index("orb")
    h, w = dom // width, dom % width
    x, core = orb // cores, orb % cores

    load_t = pltpu.make_async_copy(tile_hbm.at[pl.ds(half, n_tile)], tiles.at[dom], own_sem.at[0])
    load_t.start()
    load_o = pltpu.make_async_copy(orb_hbm, obuf.at[orb], own_sem.at[1])
    load_o.start()

    can = [h + 1 < height, h > 0, w + 1 < width, w > 0]
    to = [dom + width, dom - width, dom + 1, dom - 1]

    barrier = pltpu.get_barrier_semaphore()
    expect = n_orb - 1
    for d in range(4):
        @pl.when(can[d])
        def _(d=d):
            pl.semaphore_signal(barrier, inc=1, device_id={"dom": to[d]}, device_id_type=MESH)
        expect = expect + can[d].astype(jnp.int32)
    for d in range(1, n_orb):
        pl.semaphore_signal(barrier, inc=1, device_id={"orb": (orb + d) % n_orb}, device_id_type=MESH)
    pl.semaphore_wait(barrier, expect)
    load_t.wait()

    def tile_copy(c, origin, d):
        start, count = chunks[c]
        part = tiles.at[origin, pl.ds(start, count)]
        return pltpu.make_async_remote_copy(
            src_ref=part, dst_ref=part, send_sem=t_send.at[d, c, origin],
            recv_sem=t_recv.at[c, origin], device_id={"dom": to[d]}, device_id_type=MESH)

    def forward(c, origin, dirs):
        for d in dirs:
            @pl.when(can[d])
            def _(d=d):
                tile_copy(c, origin, d).start()

    def settle(c, origin, dirs):
        for d in dirs:
            @pl.when(can[d])
            def _(d=d):
                tile_copy(c, origin, d).wait_send()

    def arrive(c, origin):
        tile_copy(c, origin, 0).wait_recv()

    def orb_copy(k, origin, target):
        part = obuf.at[origin, k // slots, k % slots]
        return pltpu.make_async_remote_copy(
            src_ref=part, dst_ref=part, send_sem=o_send.at[origin, target, k],
            recv_sem=o_recv.at[origin, k], device_id={"orb": target}, device_id_type=MESH)

    n_orb_chunk = n_blk * slots
    far = [((x + i) % chips) * cores + core for i in range(1, chips)]
    near = [x * cores + (core + i) % cores for i in range(1, cores)]

    n_chunk = len(chunks)
    for c in range(n_chunk):
        forward(c, dom, (2, 3, 0, 1) if c == 0 else (0, 1, 2, 3))
    load_o.wait()
    for k in range(n_orb_chunk):
        for target in far:
            orb_copy(k, orb, target).start()
    for k in range(n_orb_chunk):
        for target in near:
            orb_copy(k, orb, target).start()

    def relay_orb(k):
        for origin in far:
            orb_copy(k, origin, orb).wait_recv()
            for target in near:
                orb_copy(k, origin, target).start()

    def along_width(act_plus, act_minus):
        def step(u, carry):
            @pl.when(w - u >= 0)
            def _():
                act_plus(w - u)
            @pl.when(w + u < width)
            def _():
                act_minus(w + u)
            return carry
        lax.fori_loop(1, width, step, 0)

    def first_in(ow, d):
        arrive(0, h * width + ow)
        forward(0, h * width + ow, (d, 0, 1))

    along_width(lambda ow: first_in(ow, 2), lambda ow: first_in(ow, 3))

    n_rest = n_chunk - 1
    lag = 2

    def height_step(t, carry):
        sides = ((h - t >= 0, h - t, 0), (h + t < height, h + t, 1))
        for ok, row, d in sides:
            @pl.when(ok)
            def _(row=row, d=d):
                arrive(0, row * width + w)
                forward(0, row * width + w, (d,))
        for c in range(1, n_chunk):
            for ok, row, d in sides:
                @pl.when(ok)
                def _(row=row, d=d, c=c):
                    arrive(c, row * width + w)
                    forward(c, row * width + w, (d, 2, 3))
            k = (t - 1) * n_rest + (c - 1) - lag
            @pl.when((k >= 0) & (k < n_orb_chunk))
            def _(k=k):
                relay_orb(k)
        for ok, row, d in sides:
            def other(u, carry, row=row, d=d):
                origin = row * width + (w + u) % width
                arrive(0, origin)
                forward(0, origin, (d,))
                return carry
            @pl.when(ok)
            def _(other=other):
                lax.fori_loop(1, width, other, 0)
        return carry

    lax.fori_loop(1, height, height_step, 0)
    done = max(0, (height - 1) * n_rest - lag)
    for k in range(min(done, n_orb_chunk), n_orb_chunk):
        relay_orb(k)

    def late_row(i, carry):
        row = (h + i) % height
        for c in range(1, n_chunk):
            def late(ow, d, c=c):
                arrive(c, row * width + ow)
                forward(c, row * width + ow, (d,))
            along_width(functools.partial(late, d=2), functools.partial(late, d=3))
        return carry

    def orb_in(k, carry):
        for target in near:
            orb_copy(k, target, orb).wait_recv()
            for i in range(1, chips):
                origin = ((x + i) % chips) * cores + target % cores
                orb_copy(k, origin, orb).wait_recv()
        return carry
    lax.fori_loop(0, n_orb_chunk, orb_in, 0)
    lax.fori_loop(0, height, late_row, 0)

    zero = jnp.zeros((), jnp.bfloat16)
    for g in range(n_blk):
        ids = [ids_ref[g, m] for m in range(slots)]
        live = [count_ref[g] > m for m in range(slots)]
        for m0 in range(0, slots, 2):
            targets = [m for m in (m0, m0 + 1) if m < slots]
            sources = [l for l in range(slots) if any(abs(l - m) <= half for m in targets)]
            for si, l in enumerate(sources):
                for ti, m in enumerate(targets):
                    at = (pl.ds(si * n_dom * rows, n_dom * rows), pl.ds(ti * cols, cols))
                    if abs(l - m) > half:
                        wcat[at[0], at[1]] = jnp.zeros((n_dom * rows, cols), jnp.bfloat16)
                        continue
                    offset = ids[m] - ids[l] + half
                    column = jnp.clip(offset, 0, band - 1)
                    keep = (offset >= 0) & (offset < band) & live[l] & live[m] & (pat_ref[column, ids[l]] == 1)
                    index = jnp.clip(ids[l] * band + column - half, 0, n_tile - 1)
                    picked = tiles[:, index].reshape(n_dom * rows, cols)
                    wcat[at[0], at[1]] = jnp.where(keep, picked, jnp.zeros_like(picked))
            depth = len(sources) * n_dom * rows
            block = min(1024, points)

            def piece(i, carry, g=g, m0=m0, targets=targets, sources=sources, depth=depth):
                span = pl.ds(pl.multiple_of(i * block, block), block)
                lhs = jnp.concatenate(
                    [obuf[o, g, l, span, :] for l in sources for o in range(n_orb)], axis=1)
                both = jnp.dot(lhs, wcat[pl.ds(0, depth), :], preferred_element_type=jnp.float32)
                total = None
                for ti, m in enumerate(targets):
                    part = both[:, ti * cols:(ti + 1) * cols].astype(jnp.bfloat16)
                    out_ref[g, m, span, :] = part
                    wide = part.astype(jnp.float32)
                    term = wide * wide * occ_ref[pl.ds(ids_ref[g, m], 1), :]
                    total = term if total is None else total + term
                if m0 > 0:
                    total = total + acc_ref[span, :]
                acc_ref[span, :] = total
                return carry
            lax.fori_loop(0, points // block, piece, 0)
        ones = jnp.ones((8, cols), jnp.float32)
        line = lax.dot_general(ones, acc_ref[...], (((1,), (1,)), ((), ())),
                               precision=lax.Precision.HIGHEST, preferred_element_type=jnp.float32)
        dbuf[orb, pl.ds(g, 1), :] = line[0:1, :]

    def settle_all(origin, carry):
        row, ow = origin // width, origin % width
        for c in range(n_chunk):
            if c == 0:
                dirs = ((row <= h, 0), (row >= h, 1), ((row == h) & (ow <= w), 2), ((row == h) & (ow >= w), 3))
            else:
                dirs = (((ow == w) & (row <= h), 0), ((ow == w) & (row >= h), 1), (ow <= w, 2), (ow >= w, 3))
            for sent, d in dirs:
                @pl.when(sent & can[d])
                def _(c=c, d=d):
                    tile_copy(c, origin, d).wait_send()
        return carry
    lax.fori_loop(0, n_dom, settle_all, 0)

    def settle_orb(k, carry):
        for target in far + near:
            orb_copy(k, orb, target).wait_send()
        for origin in far:
            for target in near:
                orb_copy(k, origin, target).wait_send()
        return carry
    lax.fori_loop(0, n_orb_chunk, settle_orb, 0)

    def dens_copy(origin, target):
        return pltpu.make_async_remote_copy(
            src_ref=dbuf.at[origin], dst_ref=dbuf.at[origin], send_sem=d_send.at[target],
            recv_sem=d_recv.at[origin], device_id={"orb": target}, device_id_type=MESH)
    for i in range(1, n_orb):
        dens_copy(orb, (orb + i) % n_orb).start()
    for i in range(1, n_orb):
        dens_copy((orb + i) % n_orb, orb).wait_recv()
    total = dbuf[0]
    for o in range(1, n_orb):
        total = total + dbuf[o]
    dens_ref[...] = total
    for i in range(1, n_orb):
        dens_copy(orb, (orb + i) % n_orb).wait_send()


def solution(mesh):
    n_dom, n_orb = mesh.shape["dom"], mesh.shape["orb"]
    width, cores = grid_of(mesh)
    height, chips = n_dom // width, n_orb // cores

    def local(orbitals, slot_ids, slot_count, band_tiles, pattern, occupation):
        n_blk, slots, points, cols = orbitals.shape
        blocks, band, rows, _ = band_tiles.shape
        half = (band - 1) // 2
        n_tile = blocks * band - 2 * half
        chunks = plan_chunks(n_tile, height, width)
        n_k = n_blk * slots
        depth = min(slots, 2 * half + 2) * n_dom * rows
        dma = pltpu.SemaphoreType.DMA
        vmem = pl.BlockSpec(memory_space=pltpu.VMEM)
        smem = pl.BlockSpec(memory_space=pltpu.SMEM)
        hbm = pl.BlockSpec(memory_space=pltpu.HBM)
        return pl.pallas_call(
            functools.partial(kernel, (height, width, chips, cores), chunks),
            out_shape=(
                pltpu.VMEM(orbitals.shape, jnp.bfloat16),
                pltpu.VMEM((n_blk, points), jnp.float32),
            ),
            in_specs=[hbm, hbm, smem, smem, smem, vmem],
            out_specs=(vmem, vmem),
            scratch_shapes=[
                pltpu.VMEM((n_dom, n_tile, rows, cols), jnp.bfloat16),
                pltpu.VMEM((n_orb, n_blk, slots, points, cols), jnp.bfloat16),
                pltpu.VMEM((depth, 2 * cols), jnp.bfloat16),
                pltpu.VMEM((n_orb, n_blk, points), jnp.float32),
                pltpu.VMEM((points, cols), jnp.float32),
                dma((2,)),
                dma((4, len(chunks), n_dom)),
                dma((len(chunks), n_dom)),
                dma((n_orb, n_orb, n_k)),
                dma((n_orb, n_k)),
                dma((n_orb,)),
                dma((n_orb,)),
            ],
            compiler_params=pltpu.CompilerParams(
                collective_id=0, has_side_effects=True, vmem_limit_bytes=60 * 1024 * 1024),
        )(orbitals, band_tiles.reshape(blocks * band, rows, cols), slot_ids, slot_count, pattern.T, occupation)

    placed = (
        P("dom", None, None, "orb"),
        P("dom", None),
        P("dom"),
        P(None, None, "dom", "orb"),
        P(),
        P(None, "orb"),
    )
    return jax.shard_map(
        local,
        mesh=mesh,
        in_specs=placed,
        out_specs=(P("dom", None, None, "orb"), P("dom", None)),
        check_vma=False,
    )
```

```python
import functools
import jax
import jax.numpy as jnp
from jax import lax
from jax.experimental import pallas as pl
from jax.experimental.pallas import tpu as pltpu
from jax.sharding import PartitionSpec as P

MESH = pl.DeviceIdType.MESH
CHUNKS = 4


def grid_of(mesh):
    devices = mesh.devices
    try:
        at = [tuple(d.coords) for d in devices[:, 0]]
        width = 1
        axis = [a != b for a, b in zip(at[0], at[1])].index(True)
        while width < len(at) and all(
            at[width][i] == at[0][i] + (width if i == axis else 0) for i in range(len(at[0]))
        ):
            width += 1
        first = tuple(devices[0, 0].coords)
        cores = sum(tuple(d.coords) == first for d in devices[0, :])
    except (AttributeError, IndexError, ValueError):
        width, cores = 1, 1
    if devices.shape[0] % width:
        width = 1
    if devices.shape[1] % cores:
        cores = 1
    return width, cores


def plan_chunks(total, height, width):
    first = (width - 1, (height - 1) * width)
    rest = ((width - 1) * height, height - 1)
    best = min(
        range(0, total),
        key=lambda n: max(first[i] * n + rest[i] * (total - n) for i in (0, 1)),
    ) if width > 1 else 0
    best = max(best, 1)
    chunks = [(0, best)]
    left, start = total - best, best
    for i in range(CHUNKS):
        count = left // CHUNKS + (1 if i < left % CHUNKS else 0)
        if count:
            chunks.append((start, count))
        start += count
    return chunks


def kernel(sizes, chunks, orb_hbm, tile_hbm, ids_ref, count_ref, pat_ref, occ_ref,
           out_ref, dens_ref, tiles, obuf, wcat, dbuf, acc_ref,
           own_sem, t_send, t_recv, o_send, o_recv, d_send, d_recv):
    height, width, chips, cores = sizes
    n_dom, n_tile, rows, cols = tiles.shape
    n_orb, n_blk, slots, points, _ = obuf.shape
    band = pat_ref.shape[0]
    half = (band - 1) // 2
    dom = lax.axis_index("dom")
    orb = lax.axis_index("orb")
    h, w = dom // width, dom % width
    x, core = orb // cores, orb % cores

    load_t = pltpu.make_async_copy(tile_hbm.at[pl.ds(half, n_tile)], tiles.at[dom], own_sem.at[0])
    load_t.start()
    load_o = pltpu.make_async_copy(orb_hbm, obuf.at[orb], own_sem.at[1])
    load_o.start()

    can = [h + 1 < height, h > 0, w + 1 < width, w > 0]
    to = [dom + width, dom - width, dom + 1, dom - 1]

    barrier = pltpu.get_barrier_semaphore()
    expect = n_orb - 1
    for d in range(4):
        @pl.when(can[d])
        def _(d=d):
            pl.semaphore_signal(barrier, inc=1, device_id={"dom": to[d]}, device_id_type=MESH)
        expect = expect + can[d].astype(jnp.int32)
    for d in range(1, n_orb):
        pl.semaphore_signal(barrier, inc=1, device_id={"orb": (orb + d) % n_orb}, device_id_type=MESH)
    pl.semaphore_wait(barrier, expect)
    load_t.wait()

    def tile_copy(c, origin, d):
        start, count = chunks[c]
        part = tiles.at[origin, pl.ds(start, count)]
        return pltpu.make_async_remote_copy(
            src_ref=part, dst_ref=part, send_sem=t_send.at[d, c, origin],
            recv_sem=t_recv.at[c, origin], device_id={"dom": to[d]}, device_id_type=MESH)

    def forward(c, origin, dirs):
        for d in dirs:
            @pl.when(can[d])
            def _(d=d):
                tile_copy(c, origin, d).start()

    def settle(c, origin, dirs):
        for d in dirs:
            @pl.when(can[d])
            def _(d=d):
                tile_copy(c, origin, d).wait_send()

    def arrive(c, origin):
        tile_copy(c, origin, 0).wait_recv()

    def orb_copy(k, origin, target):
        part = obuf.at[origin, k // slots, k % slots]
        return pltpu.make_async_remote_copy(
            src_ref=part, dst_ref=part, send_sem=o_send.at[origin, target, k],
            recv_sem=o_recv.at[origin, k], device_id={"orb": target}, device_id_type=MESH)

    n_orb_chunk = n_blk * slots
    far = [((x + i) % chips) * cores + core for i in range(1, chips)]
    near = [x * cores + (core + i) % cores for i in range(1, cores)]

    n_chunk = len(chunks)
    for c in range(n_chunk):
        forward(c, dom, (2, 3, 0, 1) if c == 0 else (0, 1, 2, 3))
    load_o.wait()
    for k in range(n_orb_chunk):
        for target in far:
            orb_copy(k, orb, target).start()
    for k in range(n_orb_chunk):
        for target in near:
            orb_copy(k, orb, target).start()

    def relay_orb(k):
        for origin in far:
            orb_copy(k, origin, orb).wait_recv()
            for target in near:
                orb_copy(k, origin, target).start()

    def along_width(act_plus, act_minus):
        def step(u, carry):
            @pl.when(w - u >= 0)
            def _():
                act_plus(w - u)
            @pl.when(w + u < width)
            def _():
                act_minus(w + u)
            return carry
        lax.fori_loop(1, width, step, 0)

    def first_in(ow, d):
        arrive(0, h * width + ow)
        forward(0, h * width + ow, (d, 0, 1))

    along_width(lambda ow: first_in(ow, 2), lambda ow: first_in(ow, 3))

    n_rest = n_chunk - 1
    lag = 2

    def height_step(t, carry):
        sides = ((h - t >= 0, h - t, 0), (h + t < height, h + t, 1))
        for ok, row, d in sides:
            @pl.when(ok)
            def _(row=row, d=d):
                arrive(0, row * width + w)
                forward(0, row * width + w, (d,))
        for c in range(1, n_chunk):
            for ok, row, d in sides:
                @pl.when(ok)
                def _(row=row, d=d, c=c):
                    arrive(c, row * width + w)
                    forward(c, row * width + w, (d, 2, 3))
            k = (t - 1) * n_rest + (c - 1) - lag
            @pl.when((k >= 0) & (k < n_orb_chunk))
            def _(k=k):
                relay_orb(k)
        for ok, row, d in sides:
            def other(u, carry, row=row, d=d):
                origin = row * width + (w + u) % width
                arrive(0, origin)
                forward(0, origin, (d,))
                return carry
            @pl.when(ok)
            def _(other=other):
                lax.fori_loop(1, width, other, 0)
        return carry

    lax.fori_loop(1, height, height_step, 0)
    done = max(0, (height - 1) * n_rest - lag)
    for k in range(min(done, n_orb_chunk), n_orb_chunk):
        relay_orb(k)

    def late_row(i, carry):
        row = (h + i) % height
        for c in range(1, n_chunk):
            def late(ow, d, c=c):
                arrive(c, row * width + ow)
                forward(c, row * width + ow, (d,))
            along_width(functools.partial(late, d=2), functools.partial(late, d=3))
        return carry

    def orb_in(k, carry):
        for target in near:
            orb_copy(k, target, orb).wait_recv()
            for i in range(1, chips):
                origin = ((x + i) % chips) * cores + target % cores
                orb_copy(k, origin, orb).wait_recv()
        return carry
    lax.fori_loop(0, n_orb_chunk, orb_in, 0)
    lax.fori_loop(0, height, late_row, 0)

    zero = jnp.zeros((), jnp.bfloat16)
    for g in range(n_blk):
        ids = [ids_ref[g, m] for m in range(slots)]
        live = [count_ref[g] > m for m in range(slots)]
        for m0 in range(0, slots, 2):
            slot = g * ((slots + 1) // 2) + m0 // 2
            targets = [m for m in (m0, m0 + 1) if m < slots]
            sources = [l for l in range(slots) if any(abs(l - m) <= half for m in targets)]
            for si, l in enumerate(sources):
                for ti, m in enumerate(targets):
                    at = (pl.ds(si * n_dom * rows, n_dom * rows), pl.ds(ti * cols, cols))
                    if abs(l - m) > half:
                        wcat[slot, at[0], at[1]] = jnp.zeros((n_dom * rows, cols), jnp.bfloat16)
                        continue
                    offset = ids[m] - ids[l] + half
                    column = jnp.clip(offset, 0, band - 1)
                    keep = (offset >= 0) & (offset < band) & live[l] & live[m] & (pat_ref[column, ids[l]] == 1)
                    index = jnp.clip(ids[l] * band + column - half, 0, n_tile - 1)
                    picked = tiles[:, index].reshape(n_dom * rows, cols)
                    wcat[slot, at[0], at[1]] = jnp.where(keep, picked, jnp.zeros_like(picked))
            depth = len(sources) * n_dom * rows
            block = min(1024, points)

            def piece(i, carry, g=g, m0=m0, targets=targets, sources=sources, depth=depth, slot=slot):
                span = pl.ds(0 if points == block else pl.multiple_of(i * block, block), block)
                lhs = jnp.concatenate(
                    [obuf[o, g, l, span, :] for l in sources for o in range(n_orb)], axis=1)
                both = jnp.dot(lhs, wcat[slot, pl.ds(0, depth), :], preferred_element_type=jnp.float32)
                total = None
                for ti, m in enumerate(targets):
                    part = both[:, ti * cols:(ti + 1) * cols].astype(jnp.bfloat16)
                    out_ref[g, m, span, :] = part
                    wide = part.astype(jnp.float32)
                    term = wide * wide * occ_ref[pl.ds(ids_ref[g, m], 1), :]
                    total = term if total is None else total + term
                if m0 > 0:
                    total = total + acc_ref[span, :]
                acc_ref[span, :] = total
                return carry
            if points == block:
                piece(0, 0)
            else:
                lax.fori_loop(0, points // block, piece, 0)
        ones = jnp.ones((8, cols), jnp.float32)
        line = lax.dot_general(ones, acc_ref[...], (((1,), (1,)), ((), ())),
                               precision=lax.Precision.HIGHEST, preferred_element_type=jnp.float32)
        dbuf[orb, pl.ds(g, 1), :] = line[0:1, :]

    def settle_all(origin, carry):
        row, ow = origin // width, origin % width
        for c in range(n_chunk):
            if c == 0:
                dirs = ((row <= h, 0), (row >= h, 1), ((row == h) & (ow <= w), 2), ((row == h) & (ow >= w), 3))
            else:
                dirs = (((ow == w) & (row <= h), 0), ((ow == w) & (row >= h), 1), (ow <= w, 2), (ow >= w, 3))
            for sent, d in dirs:
                @pl.when(sent & can[d])
                def _(c=c, d=d):
                    tile_copy(c, origin, d).wait_send()
        return carry
    lax.fori_loop(0, n_dom, settle_all, 0)

    def settle_orb(k, carry):
        for target in far + near:
            orb_copy(k, orb, target).wait_send()
        for origin in far:
            for target in near:
                orb_copy(k, origin, target).wait_send()
        return carry
    lax.fori_loop(0, n_orb_chunk, settle_orb, 0)

    def dens_copy(origin, target):
        return pltpu.make_async_remote_copy(
            src_ref=dbuf.at[origin], dst_ref=dbuf.at[origin], send_sem=d_send.at[target],
            recv_sem=d_recv.at[origin], device_id={"orb": target}, device_id_type=MESH)
    for i in range(1, n_orb):
        dens_copy(orb, (orb + i) % n_orb).start()
    for i in range(1, n_orb):
        dens_copy((orb + i) % n_orb, orb).wait_recv()
    total = dbuf[0]
    for o in range(1, n_orb):
        total = total + dbuf[o]
    dens_ref[...] = total
    for i in range(1, n_orb):
        dens_copy(orb, (orb + i) % n_orb).wait_send()


def solution(mesh):
    n_dom, n_orb = mesh.shape["dom"], mesh.shape["orb"]
    width, cores = grid_of(mesh)
    height, chips = n_dom // width, n_orb // cores

    def local(orbitals, slot_ids, slot_count, band_tiles, pattern, occupation):
        n_blk, slots, points, cols = orbitals.shape
        blocks, band, rows, _ = band_tiles.shape
        half = (band - 1) // 2
        n_tile = blocks * band - 2 * half
        chunks = plan_chunks(n_tile, height, width)
        n_k = n_blk * slots
        depth = min(slots, 2 * half + 2) * n_dom * rows
        dma = pltpu.SemaphoreType.DMA
        vmem = pl.BlockSpec(memory_space=pltpu.VMEM)
        smem = pl.BlockSpec(memory_space=pltpu.SMEM)
        hbm = pl.BlockSpec(memory_space=pltpu.HBM)
        return pl.pallas_call(
            functools.partial(kernel, (height, width, chips, cores), chunks),
            out_shape=(
                pltpu.VMEM(orbitals.shape, jnp.bfloat16),
                pltpu.VMEM((n_blk, points), jnp.float32),
            ),
            in_specs=[hbm, hbm, smem, smem, smem, vmem],
            out_specs=(vmem, vmem),
            scratch_shapes=[
                pltpu.VMEM((n_dom, n_tile, rows, cols), jnp.bfloat16),
                pltpu.VMEM((n_orb, n_blk, slots, points, cols), jnp.bfloat16),
                pltpu.VMEM((n_blk * ((slots + 1) // 2), depth, 2 * cols), jnp.bfloat16),
                pltpu.VMEM((n_orb, n_blk, points), jnp.float32),
                pltpu.VMEM((points, cols), jnp.float32),
                dma((2,)),
                dma((4, len(chunks), n_dom)),
                dma((len(chunks), n_dom)),
                dma((n_orb, n_orb, n_k)),
                dma((n_orb, n_k)),
                dma((n_orb,)),
                dma((n_orb,)),
            ],
            compiler_params=pltpu.CompilerParams(
                collective_id=0, has_side_effects=True, vmem_limit_bytes=60 * 1024 * 1024),
        )(orbitals, band_tiles.reshape(blocks * band, rows, cols), slot_ids, slot_count, pattern.T, occupation)

    placed = (
        P("dom", None, None, "orb"),
        P("dom", None),
        P("dom"),
        P(None, None, "dom", "orb"),
        P(),
        P(None, "orb"),
    )
    return jax.shard_map(
        local,
        mesh=mesh,
        in_specs=placed,
        out_specs=(P("dom", None, None, "orb"), P("dom", None)),
        check_vma=False,
    )
```
